256 devices in a mesh: dp: 16 (over y_hi, x, core), mp: 16 (over y_lo, z).
Axes of the slice: x: 4, y: 4 (y_hi: 2, y_lo: 2; y = y_hi * 2 + y_lo), z: 8, core: 2. Of those that a mesh axis runs over, the one named last changes fastest.
Arguments:
- grid_latent: bfloat16 [16, 4096, 1024], P('dp', 'mp'), may hold values from -6 to 6
- mesh_latent: bfloat16 [16, 2048, 1024], P('dp', 'mp'), may hold values from -6 to 6
- edge_source: int32 [16, 12288], P('dp', 'mp'), may hold values from 0 to 4095, as said below
- edge_dest: int32 [16, 12288], P('dp', 'mp'), may hold values from 0 to 2047, as said below
- edge_count: int32 [16, 16], P('dp', 'mp'), may hold values from 256 to 768, as said below
- edge_attr: float32 [16, 4, 12288], P('dp', None, 'mp'), may hold values from -5 to 5
- w_attr: float32 [4, 1024], replicated, may hold values from -3 to 3
- w_in: bfloat16 [1024, 1024], replicated, may hold values from -0.1875 to 0.1875
- w_out: bfloat16 [1024, 1024], replicated, may hold values from -0.1875 to 0.1875
- w_qkv: bfloat16 [3, 1024, 1024], P(None, None, 'mp')
- w_o: bfloat16 [1024, 1024], P('mp'), may hold values from -0.1875 to 0.1875
- cotangent: bfloat16 [16, 2048, 1024], P('dp', 'mp'), may hold values from -6 to 6
Outputs:
- d_grid: bfloat16 [16, 4096, 1024], P('dp', 'mp')
- d_mesh: bfloat16 [16, 2048, 1024], P('dp', 'mp')
- d_w_attr: float32 [4, 1024], replicated
- d_w_in: float32 [1024, 1024], P('dp', 'mp')
- d_w_out: float32 [1024, 1024], P('dp', 'mp')
- d_w_qkv: float32 [3, 1024, 1024], P(None, 'dp', 'mp')
- d_w_o: float32 [1024, 1024], P('mp', 'dp')
The draws below stay inside these ranges and needn't reach their ends.
Inputs may be any that keep to these rules, and one draw needn't show every extreme that they name: `edge_source`: edge slots of band b (positions b * 768 to (b + 1) * 768 - 1 of a sample) name grid points of band b, rows b * 256 to (b + 1) * 256 - 1. `edge_dest`: edge slots of band b name mesh nodes of band b - 1, b or b + 1 (bands of 128 nodes each). `edge_count`: the first and last bands of every sample are full.
All inputs are finite; a program needn't handle non-finite values.
Results may differ from the reference program's by a relative error of at most 0.025.
Values may be sent and summed in bfloat16 or wider, within the bound.
No kernel may reach another device: no remote copies, remote signals or barrier semaphores. Data moves between devices by JAX's collectives and lax.ppermute only.
A program may use at most 128 MiB of HBM per device.

```python
import jax
import jax.numpy as jnp
from jax import lax

C = 1024
HEADS = 16
HDIM = 64
ATTR = 4
GRID_DEV = 256
EDGES_DEV = 768
NODE_DEV = 128
SAMPLES = 16
GRID = 4096
EDGES = 12288
MESH = 2048


def draw_edge_source(key, part):
    band = jnp.arange(EDGES, dtype=jnp.int32) // EDGES_DEV
    local = jax.random.randint(jax.random.fold_in(key, 11), (SAMPLES, EDGES), 0, GRID_DEV)
    return (band[None, :] * GRID_DEV + local).astype(jnp.int32)


def draw_edge_dest(key, part):
    bands = EDGES // EDGES_DEV
    band = jnp.arange(EDGES, dtype=jnp.int32) // EDGES_DEV
    first = jax.random.fold_in(key, 23)
    second = jax.random.fold_in(key, 29)
    offset = jax.random.randint(first, (SAMPLES, EDGES), -1, 2)
    target = jnp.clip(band[None, :] + offset, 0, bands - 1)
    local = jax.random.randint(second, (SAMPLES, EDGES), 0, NODE_DEV)
    return (target * NODE_DEV + local).astype(jnp.int32)


def draw_edge_count(key, part):
    bands = EDGES // EDGES_DEV
    counts = jax.random.randint(jax.random.fold_in(key, 31), (SAMPLES, bands), EDGES_DEV // 3, EDGES_DEV + 1)
    counts = counts.at[:, 0].set(EDGES_DEV)
    counts = counts.at[:, bands - 1].set(EDGES_DEV)
    return counts.astype(jnp.int32)


def draw_w_qkv(key, part):
    base = jax.random.normal(jax.random.fold_in(key, 37), (3, C, C), jnp.float32) / jnp.sqrt(jnp.float32(C))
    return base.astype(jnp.bfloat16)


def level_of(stream_key, shape, pieces, low, top_value):
    loudness, own = 1.0, jax.random.fold_in(stream_key, 6)
    for dim, shards_of in pieces:
        draws = jnp.exp(jax.random.uniform(jax.random.fold_in(own, dim), (shards_of,), jnp.float32, low / len(pieces), top_value / len(pieces)))
        loudness = loudness * jnp.repeat(draws, shape[dim] // shards_of).reshape([-1 if axis == dim else 1 for axis in range(len(shape))])
    return loudness


def bell_draw(stream_key, extent, spread, reach, pieces=(), kind=jnp.bfloat16):
    values = jax.random.normal(stream_key, extent, jnp.float32) * spread
    if len(pieces) > 0:
        values = level_of(stream_key, extent, pieces, -0.22, 0.18) * values
    return jnp.clip(values, min=-reach, max=reach).astype(kind)


def setup_inputs(seed: int = 0) -> dict:
    streams_of = jax.random.split(jax.random.key(seed), 13)
    grid_latent = bell_draw(streams_of[0], (SAMPLES, GRID, C), 1.0, 6.0, ((0, 16), (1, 16)))
    mesh_latent = bell_draw(streams_of[1], (SAMPLES, MESH, C), 1.0, 6.0, ((0, 16), (1, 16)))
    edge_source = draw_edge_source(jax.random.fold_in(streams_of[12], 71), 0)
    edge_dest = draw_edge_dest(jax.random.fold_in(streams_of[12], 71), 0)
    edge_count = draw_edge_count(jax.random.fold_in(streams_of[12], 71), 0)
    edge_attr = bell_draw(streams_of[5], (SAMPLES, ATTR, EDGES), 1.0, 5.0, ((0, 16), (2, 16)), jnp.float32)
    w_attr = bell_draw(streams_of[6], (ATTR, C), ATTR ** -0.5, 3.0, (), jnp.float32)
    w_in = bell_draw(streams_of[7], (C, C), C ** -0.5, 0.1875)
    w_out = bell_draw(streams_of[8], (C, C), C ** -0.5, 0.1875)
    w_qkv = draw_w_qkv(jax.random.fold_in(streams_of[12], 71), 0)
    w_o = bell_draw(streams_of[10], (C, C), C ** -0.5, 0.1875, ((0, 16),))
    cotangent = bell_draw(streams_of[11], (SAMPLES, MESH, C), 1.0, 6.0, ((0, 16), (1, 16)))
    return {"grid_latent": grid_latent, "mesh_latent": mesh_latent, "edge_source": edge_source, "edge_dest": edge_dest, "edge_count": edge_count, "edge_attr": edge_attr, "w_attr": w_attr, "w_in": w_in, "w_out": w_out, "w_qkv": w_qkv, "w_o": w_o, "cotangent": cotangent}


EPS = 1e-06

def attend_head(q, k, v, d_att):
    scale = HDIM ** (-0.5)
    scores = jnp.dot(q, k.T, preferred_element_type=jnp.float32) * scale
    probs = jax.nn.softmax(scores, axis=-1)
    probs_b = probs.astype(jnp.bfloat16)
    attended = jnp.dot(probs_b, v, preferred_element_type=jnp.float32).astype(jnp.bfloat16)
    dprob = jnp.dot(d_att, v.T, preferred_element_type=jnp.float32)
    delta = lax.optimization_barrier(jnp.sum(probs * dprob, axis=-1, keepdims=True))
    dscore = (probs * (dprob - delta) * scale).astype(jnp.bfloat16)
    dq = jnp.dot(dscore, k, preferred_element_type=jnp.float32).astype(jnp.bfloat16)
    dk = jnp.dot(dscore.T, q, preferred_element_type=jnp.float32).astype(jnp.bfloat16)
    dv = jnp.dot(probs_b.T, d_att, preferred_element_type=jnp.float32).astype(jnp.bfloat16)
    return (attended, dq, dk, dv)

def one_sample(grid, mesh, source, dest, count, attr, cot, w_attr, w_in, w_out, w_qkv, w_o):
    position = jnp.arange(EDGES, dtype=jnp.int32)
    limit = jnp.take(count, position // EDGES_DEV)
    live = (position % EDGES_DEV < limit).astype(jnp.float32)[:, None]
    projected = jnp.dot(grid, w_in, preferred_element_type=jnp.float32)
    attr_terms = jnp.dot(attr.T, w_attr, precision=lax.Precision.HIGHEST, preferred_element_type=jnp.float32)
    preact = projected[source] + attr_terms
    hidden = (jax.nn.silu(preact) * live).astype(jnp.bfloat16)
    message = jnp.dot(hidden, w_out, preferred_element_type=jnp.float32).astype(jnp.bfloat16)
    gathered = jax.ops.segment_sum(message.astype(jnp.float32), dest, num_segments=MESH)
    node = mesh.astype(jnp.float32) + gathered
    inv = lax.rsqrt(lax.optimization_barrier(jnp.mean(node * node, axis=-1, keepdims=True)) + EPS)
    normed = (node * inv).astype(jnp.bfloat16)
    qkv = jnp.stack([jnp.dot(normed, w_qkv[i], preferred_element_type=jnp.float32) for i in range(3)]).astype(jnp.bfloat16)
    heads = qkv.reshape(3, MESH, HEADS, HDIM).transpose(0, 2, 1, 3)
    d_att = jnp.dot(cot, w_o.T, preferred_element_type=jnp.float32).astype(jnp.bfloat16)
    d_att = d_att.reshape(MESH, HEADS, HDIM).transpose(1, 0, 2)
    attended, dq, dk, dv = lax.map(lambda t: attend_head(t[0], t[1], t[2], t[3]), (heads[0], heads[1], heads[2], d_att))

    def joined(a):
        return a.transpose(1, 0, 2).reshape(MESH, C)
    attended = joined(attended)
    dqkv = jnp.stack([joined(dq), joined(dk), joined(dv)])
    dw_o = jnp.dot(attended.T, cot, preferred_element_type=jnp.float32)
    dw_qkv = jnp.einsum('nc,ind->icd', normed.astype(jnp.float32), dqkv.astype(jnp.float32))
    dx = jnp.dot(dqkv[0], w_qkv[0].T, preferred_element_type=jnp.float32)
    dx = dx + jnp.dot(dqkv[1], w_qkv[1].T, preferred_element_type=jnp.float32)
    dx = dx + jnp.dot(dqkv[2], w_qkv[2].T, preferred_element_type=jnp.float32)
    dnode = cot.astype(jnp.float32) + inv * dx - node * inv * inv * inv * lax.optimization_barrier(jnp.mean(dx * node, axis=-1, keepdims=True))
    d_mesh = dnode.astype(jnp.bfloat16)
    dmessage = (d_mesh[dest].astype(jnp.float32) * live).astype(jnp.bfloat16)
    dw_out = jnp.dot(hidden.T, dmessage, preferred_element_type=jnp.float32)
    dhidden = jnp.dot(dmessage, w_out.T, preferred_element_type=jnp.float32)
    sigma = jax.nn.sigmoid(preact)
    dpre = dhidden * sigma * (1.0 + preact * (1.0 - sigma)) * live
    dw_attr = jnp.dot(attr, dpre, precision=lax.Precision.HIGHEST, preferred_element_type=jnp.float32)
    dproj = jax.ops.segment_sum(dpre.astype(jnp.bfloat16).astype(jnp.float32), source, num_segments=GRID).astype(jnp.bfloat16)
    dw_in = jnp.dot(grid.T, dproj, preferred_element_type=jnp.float32)
    d_grid = jnp.dot(dproj, w_in.T, preferred_element_type=jnp.float32).astype(jnp.bfloat16)
    return (d_grid, d_mesh, dw_attr, dw_in, dw_out, dw_qkv, dw_o)

def reference(grid_latent, mesh_latent, edge_source, edge_dest, edge_count, edge_attr, w_attr, w_in, w_out, w_qkv, w_o, cotangent):

    def step(carry, item):
        grid, mesh, source, dest, count, attr, cot = item
        d_grid, d_mesh, dw_attr, dw_in, dw_out, dw_qkv, dw_o = one_sample(grid, mesh, source, dest, count, attr, cot, w_attr, w_in, w_out, w_qkv, w_o)
        carry = (carry[0] + dw_attr, carry[1] + dw_in, carry[2] + dw_out, carry[3] + dw_qkv, carry[4] + dw_o)
        return (carry, (d_grid, d_mesh))
    start = (jnp.zeros((ATTR, C), jnp.float32), jnp.zeros((C, C), jnp.float32), jnp.zeros((C, C), jnp.float32), jnp.zeros((3, C, C), jnp.float32), jnp.zeros((C, C), jnp.float32))
    totals, outs = lax.scan(step, start, (grid_latent, mesh_latent, edge_source, edge_dest, edge_count, edge_attr, cotangent))
    return (outs[0], outs[1], totals[0], totals[1], totals[2], totals[3], totals[4])
```

```python
import functools

import jax
import jax.numpy as jnp
from jax import lax
from jax.experimental import pallas as pl
from jax.experimental.pallas import tpu as pltpu
from jax.sharding import Mesh
from jax.sharding import PartitionSpec as P

HDIM = 64
SCALE = HDIM ** (-0.5)
MP = ("mp_0", "mp_1")
DP = ("dp_0", "dp_1", "dp_2")
GROUP = ("dp_0", "dp_1")
CORE = "dp_2"
EPS = 1e-06
BF = jnp.bfloat16
F32 = jnp.float32
NN = (((1,), (0,)), ((), ()))
NT = (((1,), (1,)), ((), ()))
TN = (((0,), (0,)), ((), ()))


def dot(a, b, dims):
    return lax.dot_general(a, b, dims, preferred_element_type=F32)


def shifted(block, axis, distance):
    devices = range(lax.axis_size(axis))
    route = [(i - distance, i) for i in devices if i - distance in devices]
    return lax.ppermute(block, axis, route)


def swapped(block):
    return lax.ppermute(block, CORE, [(0, 1), (1, 0)])


def after(value, earlier):
    return lax.optimization_barrier((value, earlier))[0]


def both_halves(mine, other, core):
    low = jnp.where(core == 0, mine, other)
    high = jnp.where(core == 0, other, mine)
    return jnp.concatenate([low, high], axis=1)


def column_half(value, half):
    width = value.shape[1] // 2
    return lax.dynamic_slice_in_dim(value, half * width, width, 1)


def attend_kernel(qkv_ref, da_ref, out_ref, k_s, v_s, kt_s, vt_s, dk_s, dv_s, *, block, steps):
    i = pl.program_id(0)

    @pl.when(i == 0)
    def _():
        k = qkv_ref[:, HDIM : 2 * HDIM]
        v = qkv_ref[:, 2 * HDIM : 3 * HDIM]
        k_s[...] = k
        v_s[...] = v
        kt_s[...] = k.T
        vt_s[...] = v.T
        dk_s[...] = jnp.zeros_like(dk_s)
        dv_s[...] = jnp.zeros_like(dv_s)

    rows = pl.ds(pl.multiple_of(i * block, block), block)
    q = qkv_ref[rows, 0:HDIM] * jnp.asarray(SCALE, BF)
    da = da_ref[rows, :]
    s = dot(k_s[...], q, NT)
    dp = dot(v_s[...], da, NT)
    e = jnp.exp(s - jnp.max(s, axis=0, keepdims=True))
    p = e * (1.0 / jnp.sum(e, axis=0, keepdims=True))
    delta = jnp.sum(p * dp, axis=0, keepdims=True)
    pb = p.astype(BF)
    ds = (p * (dp - delta)).astype(BF)
    out_ref[3 * HDIM : 4 * HDIM, rows] = dot(vt_s[...], pb, NN).astype(BF)
    out_ref[0:HDIM, rows] = (dot(kt_s[...], ds, NN) * SCALE).astype(BF)
    dk_s[...] += dot(ds, q, NN)
    dv_s[...] += dot(pb, da, NN)

    @pl.when(i == steps - 1)
    def _():
        out_ref[HDIM : 2 * HDIM, :] = dk_s[...].T.astype(BF)
        out_ref[2 * HDIM : 3 * HDIM, :] = dv_s[...].T.astype(BF)


def attend(qkv, da):
    total = qkv.shape[0]
    block = min(512, total)
    steps = total // block
    return pl.pallas_call(
        functools.partial(attend_kernel, block=block, steps=steps),
        grid=(steps,),
        in_specs=[
            pl.BlockSpec((total, 3 * HDIM), lambda i: (0, 0)),
            pl.BlockSpec((total, HDIM), lambda i: (0, 0)),
        ],
        out_specs=pl.BlockSpec((4 * HDIM, total), lambda i: (0, 0)),
        out_shape=jax.ShapeDtypeStruct((4 * HDIM, total), BF),
        scratch_shapes=[
            pltpu.VMEM((total, HDIM), BF),
            pltpu.VMEM((total, HDIM), BF),
            pltpu.VMEM((HDIM, total), BF),
            pltpu.VMEM((HDIM, total), BF),
            pltpu.VMEM((total, HDIM), F32),
            pltpu.VMEM((total, HDIM), F32),
        ],
        compiler_params=pltpu.CompilerParams(dimension_semantics=("arbitrary",)),
        cost_estimate=pl.CostEstimate(
            flops=24 * total * total * HDIM,
            transcendentals=total * total,
            bytes_accessed=20 * total * HDIM,
        ),
        name="attend",
    )(qkv, da)


def shards(
    grid_latent,
    mesh_latent,
    edge_source,
    edge_dest,
    edge_count,
    edge_attr,
    w_attr,
    w_in,
    w_out,
    w_qkv,
    w_o,
    cotangent,
):
    band = lax.axis_index(MP)
    core = lax.axis_index(CORE)
    bands = lax.axis_size(MP)
    groups = lax.axis_size(GROUP)
    grid_rows = grid_latent.shape[1]
    nodes = mesh_latent.shape[1]
    edges = edge_source.shape[1]
    channels = grid_latent.shape[2]
    grid = grid_latent[0]
    cot = cotangent[0]
    live = (jnp.arange(edges, dtype=jnp.int32) < edge_count[0, 0]).astype(F32)[:, None]
    source_local = edge_source[0] - band * grid_rows
    dest_local = edge_dest[0] - (band - 1) * nodes

    o_mine = lax.all_gather(column_half(w_o, core), MP, axis=0, tiled=True)
    o_other = swapped(o_mine)

    projected = dot(grid, w_in, NN)
    attr_columns = edge_attr[0].T
    attr_terms = sum(
        attr_columns[:, a : a + 1] * w_attr[a : a + 1] for a in range(w_attr.shape[0])
    )
    preact = projected[source_local] + attr_terms
    hidden = (jax.nn.silu(preact) * live).astype(BF)
    message = dot(hidden, w_out, NN).astype(BF)
    dest_table = (dest_local[:, None] == jnp.arange(3 * nodes, dtype=jnp.int32)[None, :]).astype(BF)
    partial_rows = dot(dest_table, message, TN)
    from_below = shifted(partial_rows[2 * nodes :].astype(BF), MP, 1)
    from_above = shifted(partial_rows[:nodes].astype(BF), MP, -1)
    node = (
        mesh_latent[0].astype(F32)
        + partial_rows[nodes : 2 * nodes]
        + from_below.astype(F32)
        + from_above.astype(F32)
    )
    inv = lax.rsqrt(jnp.mean(node * node, axis=-1, keepdims=True) + EPS)
    normed = (node * inv).astype(BF)
    all_normed = lax.all_gather(normed, MP, axis=0, tiled=True)

    d_att = (
        dot(column_half(cot, core), o_mine, NT) + dot(column_half(cot, 1 - core), o_other, NT)
    ).astype(BF)
    width = w_qkv.shape[2]
    d_att = d_att.reshape(2, nodes // 2, bands, width).transpose(2, 1, 0, 3)
    d_att = d_att.reshape(bands, nodes // 2, 2 * width)
    d_att = lax.all_to_all(d_att, MP, 0, 0, tiled=True)
    d_att = d_att.reshape(bands, nodes // 2, 2, width).transpose(0, 2, 1, 3)
    d_att = d_att.reshape(bands * nodes, width)

    w_rows = jnp.concatenate([w_qkv[0], w_qkv[1], w_qkv[2]], axis=1)
    qkv = dot(all_normed, w_rows, NN).astype(BF)
    result = attend(qkv, d_att)
    dqkv = result[: 3 * width]

    w_heads = w_qkv.transpose(0, 2, 1).reshape(3 * width, channels)
    w_half = after(column_half(w_heads, core), all_normed)
    w_mine = lax.all_gather(w_half, MP, axis=0, tiled=True)
    w_other = swapped(w_mine)
    pieces = dqkv.reshape(3 * width, bands, nodes).transpose(1, 0, 2)
    pieces = lax.all_to_all(pieces, MP, 0, 0, tiled=True)
    pieces = pieces.reshape(bands * 3 * width, nodes)
    dx = both_halves(dot(pieces, w_mine, TN), dot(pieces, w_other, TN), core)

    all_cot = lax.all_gather(after(cot, w_mine), MP, axis=0, tiled=True)

    dnode = (
        cot.astype(F32)
        + inv * dx
        - node * inv * inv * inv * jnp.mean(dx * node, axis=-1, keepdims=True)
    )
    d_mesh = dnode.astype(BF)
    low = shifted(d_mesh, MP, 1)
    high = shifted(d_mesh, MP, -1)
    beside_all = jnp.concatenate([low, d_mesh, high], axis=0)
    dmessage = (beside_all[dest_local].astype(F32) * live).astype(BF)
    dw_out = dot(hidden, dmessage, TN).astype(BF)
    dhidden = dot(dmessage, w_out, NT)
    sigma = jax.nn.sigmoid(preact)
    dpre = dhidden * sigma * (1.0 + preact * (1.0 - sigma)) * live
    dw_attr = jnp.dot(
        edge_attr[0], dpre, precision=lax.Precision.HIGHEST, preferred_element_type=F32
    )
    source_table = (
        source_local[:, None] == jnp.arange(grid_rows, dtype=jnp.int32)[None, :]
    ).astype(BF)
    dproj = dot(source_table, dpre.astype(BF), TN).astype(BF)
    dw_in = dot(grid, dproj, TN).astype(BF)
    d_grid = dot(dproj, w_in, NT).astype(BF)

    dw_x = dot(all_normed, dqkv, (((0,), (1,)), ((), ())))
    dw_c = dot(all_cot, result[3 * width :], (((0,), (1,)), ((), ())))
    dw_heads = jnp.concatenate([dw_x, dw_c], axis=1).astype(BF)
    dw_heads = dw_heads.reshape(2 * groups, -1, 4 * width)
    dw_heads = lax.all_to_all(dw_heads, DP, 0, 0, tiled=True)
    sum_heads = jnp.sum(dw_heads.astype(F32), axis=0)
    sum_qkv = jnp.stack([sum_heads[:, j * width : (j + 1) * width] for j in range(3)])
    sum_o = sum_heads[:, 3 * width :].T

    rows = channels // (2 * groups)
    both = jnp.stack(
        [dw_in.reshape(groups, 2, rows, channels), dw_out.reshape(groups, 2, rows, channels)],
        axis=2,
    )
    mine = lax.dynamic_index_in_dim(both, core, 1, keepdims=False)
    theirs = lax.dynamic_index_in_dim(both, 1 - core, 1, keepdims=False)
    pair = mine.astype(F32) + swapped(theirs).astype(F32)
    pair = pair.astype(BF).reshape(groups, 2 * rows, channels)
    attr = dw_attr + swapped(dw_attr)
    attr_rows = attr.shape[0]
    attr_high = attr.astype(BF)
    attr_low = (attr - attr_high.astype(F32)).astype(BF)
    blank = jnp.zeros((16 - 2 * attr_rows, channels), BF)
    tail = jnp.concatenate([attr_high, attr_low, blank], axis=0)
    pair = jnp.concatenate([pair, jnp.broadcast_to(tail[None], (groups, 16, channels))], axis=1)
    pair = lax.all_to_all(pair, GROUP, 0, 0, tiled=True)
    summed = jnp.sum(pair.astype(F32), axis=0)
    attr = summed[2 * rows : 2 * rows + attr_rows]
    attr = attr + summed[2 * rows + attr_rows : 2 * rows + 2 * attr_rows]
    cols = channels // bands
    blocks = summed[: 2 * rows].astype(BF).reshape(2, rows, bands, cols)
    blocks = blocks.transpose(2, 1, 0, 3).reshape(bands, rows, 2 * cols)
    tail = attr.astype(BF).reshape(1, -1, 2 * cols)
    tail = jnp.broadcast_to(tail, (bands,) + tail.shape[1:])
    blocks = jnp.concatenate([blocks, tail], axis=1)
    blocks = lax.all_to_all(blocks, MP, 0, 0, tiled=True)
    summed = jnp.sum(blocks.astype(F32), axis=0)
    sum_in = summed[:rows, :cols]
    sum_out = summed[:rows, cols:]
    sum_attr = summed[rows:].reshape(attr.shape)
    return (d_grid[None], d_mesh[None], sum_attr, sum_in, sum_out, sum_qkv, sum_o)


def solution(mesh):
    finer = Mesh(mesh.devices.reshape(2, 4, 2, 2, 8), ("dp_0", "dp_1", "dp_2", "mp_0", "mp_1"))
    in_specs = (
        P(DP, MP, None),
        P(DP, MP, None),
        P(DP, MP),
        P(DP, MP),
        P(DP, MP),
        P(DP, None, MP),
        P(),
        P(),
        P(),
        P(None, None, MP),
        P(MP, None),
        P(DP, MP, None),
    )
    out_specs = (
        P(DP, MP, None),
        P(DP, MP, None),
        P(),
        P(DP, MP),
        P(DP, MP),
        P(None, DP, MP),
        P(MP, DP),
    )
    return jax.shard_map(
        shards, mesh=finer, in_specs=in_specs, out_specs=out_specs, check_vma=False
    )
```

```python
import functools

import jax
import jax.numpy as jnp
from jax import lax
from jax.experimental import pallas as pl
from jax.experimental.pallas import tpu as pltpu
from jax.sharding import Mesh
from jax.sharding import PartitionSpec as P

HDIM = 64
SCALE = HDIM ** (-0.5)
MP = ("mp_0", "mp_1")
DP = ("dp_0", "dp_1", "dp_2")
GROUP = ("dp_0", "dp_1")
CORE = "dp_2"
EPS = 1e-06
BF = jnp.bfloat16
F32 = jnp.float32
NN = (((1,), (0,)), ((), ()))
NT = (((1,), (1,)), ((), ()))
TN = (((0,), (0,)), ((), ()))


def dot(a, b, dims):
    return lax.dot_general(a, b, dims, preferred_element_type=F32)


def shifted(block, axis, distance):
    devices = range(lax.axis_size(axis))
    route = [(i - distance, i) for i in devices if i - distance in devices]
    return lax.ppermute(block, axis, route)


def swapped(block):
    return lax.ppermute(block, CORE, [(0, 1), (1, 0)])


def after(value, earlier):
    return lax.optimization_barrier((value, earlier))[0]


def both_halves(mine, other, core):
    low = jnp.where(core == 0, mine, other)
    high = jnp.where(core == 0, other, mine)
    return jnp.concatenate([low, high], axis=1)


def column_half(value, half):
    width = value.shape[1] // 2
    return lax.dynamic_slice_in_dim(value, half * width, width, 1)


def attend_kernel(
    half_ref, qkvd_ref, out_ref, sent_ref, k_s, v_s, kt_s, vt_s, dk_s, dv_s, *, block, steps, nodes
):
    i = pl.program_id(0)
    along = block * steps // nodes // 2

    def place(b):
        position = (b % along) * 2 + (b // along + half_ref[0]) % 2
        return pl.ds(pl.multiple_of(position * nodes, nodes), nodes)

    @pl.when(i == 0)
    def _():
        k = qkvd_ref[:, HDIM : 2 * HDIM]
        v = qkvd_ref[:, 2 * HDIM : 3 * HDIM]
        k_s[...] = k
        v_s[...] = v
        kt_s[...] = k.T
        vt_s[...] = v.T
        dk_s[...] = jnp.zeros_like(dk_s)
        dv_s[...] = jnp.zeros_like(dv_s)

    rows = pl.ds(pl.multiple_of(i * block, block), block)
    q = qkvd_ref[rows, 0:HDIM] * jnp.asarray(SCALE, BF)
    da = qkvd_ref[rows, 3 * HDIM : 4 * HDIM]
    s = dot(k_s[...], q, NT)
    dp = dot(v_s[...], da, NT)
    e = jnp.exp(s - jnp.max(s, axis=0, keepdims=True))
    p = e * (1.0 / jnp.sum(e, axis=0, keepdims=True))
    delta = jnp.sum(p * dp, axis=0, keepdims=True)
    pb = p.astype(BF)
    ds = (p * (dp - delta)).astype(BF)
    attended = dot(vt_s[...], pb, NN).astype(BF)
    dq = (dot(kt_s[...], ds, NN) * SCALE).astype(BF)
    for j in range(block // nodes):
        b = i * (block // nodes) + j
        cols = slice(j * nodes, (j + 1) * nodes)
        sent_ref[b, 0:HDIM, :] = dq[:, cols]
        out_ref[0:HDIM, place(b)] = dq[:, cols]
        out_ref[3 * HDIM : 4 * HDIM, place(b)] = attended[:, cols]
    dk_s[...] += dot(ds, q, NN)
    dv_s[...] += dot(pb, da, NN)

    @pl.when(i == steps - 1)
    def _():
        dk = dk_s[...].T.astype(BF)
        dv = dv_s[...].T.astype(BF)
        for b in range(block * steps // nodes):
            cols = slice(b * nodes, (b + 1) * nodes)
            for first, value in ((HDIM, dk[:, cols]), (2 * HDIM, dv[:, cols])):
                sent_ref[b, first : first + HDIM, :] = value
                out_ref[first : first + HDIM, place(b)] = value


def attend(qkvd, half, nodes):
    total = qkvd.shape[0]
    block = min(512, total)
    steps = total // block
    return pl.pallas_call(
        functools.partial(attend_kernel, block=block, steps=steps, nodes=nodes),
        grid=(steps,),
        in_specs=[
            pl.BlockSpec(memory_space=pltpu.SMEM),
            pl.BlockSpec((total, 4 * HDIM), lambda i: (0, 0)),
        ],
        out_specs=[
            pl.BlockSpec((4 * HDIM, total), lambda i: (0, 0)),
            pl.BlockSpec((total // nodes, 3 * HDIM, nodes), lambda i: (0, 0, 0)),
        ],
        out_shape=[
            jax.ShapeDtypeStruct((4 * HDIM, total), BF),
            jax.ShapeDtypeStruct((total // nodes, 3 * HDIM, nodes), BF),
        ],
        scratch_shapes=[
            pltpu.VMEM((total, HDIM), BF),
            pltpu.VMEM((total, HDIM), BF),
            pltpu.VMEM((HDIM, total), BF),
            pltpu.VMEM((HDIM, total), BF),
            pltpu.VMEM((total, HDIM), F32),
            pltpu.VMEM((total, HDIM), F32),
        ],
        compiler_params=pltpu.CompilerParams(dimension_semantics=("arbitrary",)),
        cost_estimate=pl.CostEstimate(
            flops=24 * total * total * HDIM,
            transcendentals=total * total,
            bytes_accessed=20 * total * HDIM,
        ),
        name="attend",
    )(half.reshape(1), qkvd)


def shards(
    grid_latent,
    mesh_latent,
    edge_source,
    edge_dest,
    edge_count,
    edge_attr,
    w_attr,
    w_in,
    w_out,
    w_qkv,
    w_o,
    cotangent,
):
    band = lax.axis_index(MP)
    core = lax.axis_index(CORE)
    bands = lax.axis_size(MP)
    groups = lax.axis_size(GROUP)
    grid_rows = grid_latent.shape[1]
    nodes = mesh_latent.shape[1]
    edges = edge_source.shape[1]
    channels = grid_latent.shape[2]
    grid = grid_latent[0]
    cot = cotangent[0]
    live = (jnp.arange(edges, dtype=jnp.int32) < edge_count[0, 0]).astype(F32)[:, None]
    source_local = edge_source[0] - band * grid_rows
    dest_local = edge_dest[0] - (band - 1) * nodes

    width = w_qkv.shape[2]
    upper = lax.axis_index("dp_0")
    w_rows = jnp.concatenate([w_qkv.transpose(0, 2, 1).reshape(3 * width, channels), w_o], axis=0)
    w_part = lax.dynamic_slice_in_dim(column_half(w_rows, core), upper * 2 * width, 2 * width, 0)
    w_mine = lax.all_gather(w_part, ("dp_0",) + MP, axis=0, tiled=True)
    cot_beside = lax.ppermute(cot, "mp_0", [(0, 1), (1, 0)])

    projected = dot(grid, w_in, NN)
    attr_columns = edge_attr[0].T
    attr_terms = sum(
        attr_columns[:, a : a + 1] * w_attr[a : a + 1] for a in range(w_attr.shape[0])
    )
    preact = projected[source_local] + attr_terms
    hidden = (jax.nn.silu(preact) * live).astype(BF)
    message = dot(hidden, w_out, NN).astype(BF)
    dest_table = (dest_local[:, None] == jnp.arange(3 * nodes, dtype=jnp.int32)[None, :]).astype(BF)
    partial_rows = dot(dest_table, message, TN)
    from_below = shifted(partial_rows[2 * nodes :].astype(BF), MP, 1)
    from_above = shifted(partial_rows[:nodes].astype(BF), MP, -1)
    node = (
        mesh_latent[0].astype(F32)
        + partial_rows[nodes : 2 * nodes]
        + from_below.astype(F32)
        + from_above.astype(F32)
    )
    inv = lax.rsqrt(jnp.mean(node * node, axis=-1, keepdims=True) + EPS)
    normed = (node * inv).astype(BF)

    normed_beside = lax.ppermute(normed, "mp_0", [(0, 1), (1, 0)])
    w_mine = after(w_mine, normed_beside)
    w_other = swapped(w_mine)
    both = jnp.concatenate([normed, cot], axis=0)
    heads = dot(column_half(both, core), w_mine, NT) + dot(column_half(both, 1 - core), w_other, NT)
    column = lax.broadcasted_iota(jnp.int32, (nodes, heads.shape[1]), 1)
    of_output = (column >= 2 * width * bands) & (column % (2 * width) >= width)
    heads = jnp.where(of_output, heads[nodes:], heads[:nodes]).astype(BF)
    heads = heads.reshape(nodes, 2, bands, 2 * width).transpose(2, 0, 1, 3)
    heads = heads.reshape(bands, nodes, 4 * width)
    heads = lax.all_to_all(heads, MP, 0, 0, tiled=True).reshape(bands * nodes, 4 * width)

    wide = jnp.concatenate([normed, cot], axis=1)
    beside = jnp.concatenate([normed_beside, cot_beside], axis=1)
    wide = after(jnp.concatenate([wide, beside], axis=0), w_mine)
    wide = lax.all_gather(wide, "mp_1", axis=0, tiled=True)

    result, pieces = attend(heads, lax.axis_index("mp_0"), nodes)

    pieces = lax.all_to_all(pieces, MP, 0, 0, tiled=True)
    pieces = pieces.reshape(bands * 3 * width, nodes)

    def only_qkv(rows):
        rows = rows.reshape(2, bands, 2 * width, -1)
        rows = jnp.concatenate([rows[0], rows[1, :, :width]], axis=1)
        return rows.reshape(bands * 3 * width, -1)

    dx = both_halves(
        dot(pieces, only_qkv(w_mine), TN), dot(pieces, only_qkv(w_other), TN), core
    )

    dnode = (
        cot.astype(F32)
        + inv * dx
        - node * inv * inv * inv * jnp.mean(dx * node, axis=-1, keepdims=True)
    )
    d_mesh = dnode.astype(BF)
    low = shifted(d_mesh, MP, 1)
    high = shifted(d_mesh, MP, -1)
    beside_all = jnp.concatenate([low, d_mesh, high], axis=0)
    dmessage = (beside_all[dest_local].astype(F32) * live).astype(BF)
    dw_out = dot(hidden, dmessage, TN).astype(BF)
    dhidden = dot(dmessage, w_out, NT)
    sigma = jax.nn.sigmoid(preact)
    dpre = dhidden * sigma * (1.0 + preact * (1.0 - sigma)) * live
    dw_attr = jnp.dot(
        edge_attr[0], dpre, precision=lax.Precision.HIGHEST, preferred_element_type=F32
    )
    source_table = (
        source_local[:, None] == jnp.arange(grid_rows, dtype=jnp.int32)[None, :]
    ).astype(BF)
    dproj = dot(source_table, dpre.astype(BF), TN).astype(BF)
    dw_in = dot(grid, dproj, TN).astype(BF)
    d_grid = dot(dproj, w_in, NT).astype(BF)

    dw_heads = dot(wide, result, (((0,), (1,)), ((), ()))).astype(BF)
    of_output = lax.broadcasted_iota(jnp.int32, (channels, 4 * width), 1) >= 3 * width
    dw_heads = jnp.where(of_output, dw_heads[channels:], dw_heads[:channels])

    rows = channels // (2 * groups)
    folded = 4 * width * rows // channels
    dw_heads = dw_heads.reshape(groups, 2, rows // folded, folded, 4 * width)
    dw_heads = dw_heads.transpose(0, 1, 3, 2, 4).reshape(groups, 2, folded, channels)
    both = jnp.concatenate(
        [
            dw_in.reshape(groups, 2, rows, channels),
            dw_out.reshape(groups, 2, rows, channels),
            dw_heads,
        ],
        axis=2,
    )
    mine = lax.dynamic_index_in_dim(both, core, 1, keepdims=False)
    theirs = lax.dynamic_index_in_dim(both, 1 - core, 1, keepdims=False)
    pair = mine.astype(F32) + swapped(theirs).astype(F32)
    pair = pair.astype(BF)
    attr = dw_attr + swapped(dw_attr)
    attr_rows = attr.shape[0]
    attr_high = attr.astype(BF)
    attr_low = (attr - attr_high.astype(F32)).astype(BF)
    blank = jnp.zeros((16 - 2 * attr_rows, channels), BF)
    tail = jnp.concatenate([attr_high, attr_low, blank], axis=0)
    pair = jnp.concatenate([pair, jnp.broadcast_to(tail[None], (groups, 16, channels))], axis=1)
    pair = lax.all_to_all(pair, GROUP, 0, 0, tiled=True)
    summed = jnp.sum(pair.astype(F32), axis=0)
    sum_heads = summed[2 * rows : 2 * rows + folded]
    sum_heads = sum_heads.reshape(folded, rows // folded, 4 * width).transpose(1, 0, 2)
    sum_heads = sum_heads.reshape(rows, 4 * width)
    sum_qkv = jnp.stack([sum_heads[:, j * width : (j + 1) * width] for j in range(3)])
    sum_o = sum_heads[:, 3 * width :].T
    first = 2 * rows + folded
    attr = summed[first : first + attr_rows] + summed[first + attr_rows : first + 2 * attr_rows]
    cols = channels // bands
    blocks = summed[: 2 * rows].astype(BF).reshape(2, rows, bands, cols)
    blocks = blocks.transpose(2, 1, 0, 3).reshape(bands, rows, 2 * cols)
    tail = attr.astype(BF).reshape(1, -1, 2 * cols)
    tail = jnp.broadcast_to(tail, (bands,) + tail.shape[1:])
    blocks = jnp.concatenate([blocks, tail], axis=1)
    blocks = lax.all_to_all(blocks, MP, 0, 0, tiled=True)
    summed = jnp.sum(blocks.astype(F32), axis=0)
    sum_in = summed[:rows, :cols]
    sum_out = summed[:rows, cols:]
    sum_attr = summed[rows:].reshape(attr.shape)
    return (d_grid[None], d_mesh[None], sum_attr, sum_in, sum_out, sum_qkv, sum_o)


def solution(mesh):
    finer = Mesh(mesh.devices.reshape(2, 4, 2, 2, 8), ("dp_0", "dp_1", "dp_2", "mp_0", "mp_1"))
    in_specs = (
        P(DP, MP, None),
        P(DP, MP, None),
        P(DP, MP),
        P(DP, MP),
        P(DP, MP),
        P(DP, None, MP),
        P(),
        P(),
        P(),
        P(None, None, MP),
        P(MP, None),
        P(DP, MP, None),
    )
    out_specs = (
        P(DP, MP, None),
        P(DP, MP, None),
        P(),
        P(DP, MP),
        P(DP, MP),
        P(None, DP, MP),
        P(MP, DP),
    )
    return jax.shard_map(
        shards, mesh=finer, in_specs=in_specs, out_specs=out_specs, check_vma=False
    )
```

```python
import functools

import jax
import jax.numpy as jnp
from jax import lax
from jax.experimental import pallas as pl
from jax.experimental.pallas import tpu as pltpu
from jax.sharding import Mesh
from jax.sharding import PartitionSpec as P

HDIM = 64
SCALE = HDIM ** (-0.5)
MP = ("mp_0", "mp_1")
DP = ("dp_0", "dp_1", "dp_2")
GROUP = ("dp_0", "dp_1")
CORE = "dp_2"
EPS = 1e-06
BF = jnp.bfloat16
F32 = jnp.float32
NN = (((1,), (0,)), ((), ()))
NT = (((1,), (1,)), ((), ()))
TN = (((0,), (0,)), ((), ()))


def dot(a, b, dims):
    return lax.dot_general(a, b, dims, preferred_element_type=F32)


def shifted(block, axis, distance):
    devices = range(lax.axis_size(axis))
    route = [(i - distance, i) for i in devices if i - distance in devices]
    return lax.ppermute(block, axis, route)


def swapped(block):
    return lax.ppermute(block, CORE, [(0, 1), (1, 0)])


def after(value, earlier):
    return lax.optimization_barrier((value, earlier))[0]


def both_halves(mine, other, core):
    low = jnp.where(core == 0, mine, other)
    high = jnp.where(core == 0, other, mine)
    return jnp.concatenate([low, high], axis=1)


def column_half(value, half):
    width = value.shape[1] // 2
    return lax.dynamic_slice_in_dim(value, half * width, width, 1)


def attend_kernel(
    half_ref, qkvd_ref, out_ref, sent_ref, k_s, v_s, kt_s, vt_s, dk_s, dv_s, *, block, steps, nodes
):
    i = pl.program_id(0)
    along = block * steps // nodes // 2

    def place(b):
        position = (b % along) * 2 + (b // along + half_ref[0]) % 2
        return pl.ds(pl.multiple_of(position * nodes, nodes), nodes)

    @pl.when(i == 0)
    def _():
        k = qkvd_ref[:, HDIM : 2 * HDIM]
        v = qkvd_ref[:, 2 * HDIM : 3 * HDIM]
        k_s[...] = k
        v_s[...] = v
        kt_s[...] = k.T
        vt_s[...] = v.T
        dk_s[...] = jnp.zeros_like(dk_s)
        dv_s[...] = jnp.zeros_like(dv_s)

    rows = pl.ds(pl.multiple_of(i * block, block), block)
    q = qkvd_ref[rows, 0:HDIM] * jnp.asarray(SCALE, BF)
    da = qkvd_ref[rows, 3 * HDIM : 4 * HDIM]
    s = dot(k_s[...], q, NT)
    dp = dot(v_s[...], da, NT)
    e = jnp.exp(s - jnp.max(s, axis=0, keepdims=True))
    p = e * (1.0 / jnp.sum(e, axis=0, keepdims=True))
    delta = jnp.sum(p * dp, axis=0, keepdims=True)
    pb = p.astype(BF)
    ds = (p * (dp - delta)).astype(BF)
    attended = dot(vt_s[...], pb, NN).astype(BF)
    dq = (dot(kt_s[...], ds, NN) * SCALE).astype(BF)
    for j in range(block // nodes):
        b = i * (block // nodes) + j
        cols = slice(j * nodes, (j + 1) * nodes)
        sent_ref[b, 0:HDIM, :] = dq[:, cols]
        out_ref[0:HDIM, place(b)] = dq[:, cols]
        out_ref[3 * HDIM : 4 * HDIM, place(b)] = attended[:, cols]
    dk_s[...] += dot(ds, q, NN)
    dv_s[...] += dot(pb, da, NN)

    @pl.when(i == steps - 1)
    def _():
        dk = dk_s[...].T.astype(BF)
        dv = dv_s[...].T.astype(BF)
        for b in range(block * steps // nodes):
            cols = slice(b * nodes, (b + 1) * nodes)
            for first, value in ((HDIM, dk[:, cols]), (2 * HDIM, dv[:, cols])):
                sent_ref[b, first : first + HDIM, :] = value
                out_ref[first : first + HDIM, place(b)] = value


def attend(qkvd, half, nodes):
    total = qkvd.shape[0]
    block = min(512, total)
    steps = total // block
    return pl.pallas_call(
        functools.partial(attend_kernel, block=block, steps=steps, nodes=nodes),
        grid=(steps,),
        in_specs=[
            pl.BlockSpec(memory_space=pltpu.SMEM),
            pl.BlockSpec((total, 4 * HDIM), lambda i: (0, 0)),
        ],
        out_specs=[
            pl.BlockSpec((4 * HDIM, total), lambda i: (0, 0)),
            pl.BlockSpec((total // nodes, 3 * HDIM, nodes), lambda i: (0, 0, 0)),
        ],
        out_shape=[
            jax.ShapeDtypeStruct((4 * HDIM, total), BF),
            jax.ShapeDtypeStruct((total // nodes, 3 * HDIM, nodes), BF),
        ],
        scratch_shapes=[
            pltpu.VMEM((total, HDIM), BF),
            pltpu.VMEM((total, HDIM), BF),
            pltpu.VMEM((HDIM, total), BF),
            pltpu.VMEM((HDIM, total), BF),
            pltpu.VMEM((total, HDIM), F32),
            pltpu.VMEM((total, HDIM), F32),
        ],
        compiler_params=pltpu.CompilerParams(dimension_semantics=("arbitrary",)),
        cost_estimate=pl.CostEstimate(
            flops=24 * total * total * HDIM,
            transcendentals=total * total,
            bytes_accessed=20 * total * HDIM,
        ),
        name="attend",
    )(half.reshape(1), qkvd)


def shards(
    grid_latent,
    mesh_latent,
    edge_source,
    edge_dest,
    edge_count,
    edge_attr,
    w_attr,
    w_in,
    w_out,
    w_qkv,
    w_o,
    cotangent,
):
    band = lax.axis_index(MP)
    core = lax.axis_index(CORE)
    bands = lax.axis_size(MP)
    groups = lax.axis_size(GROUP)
    grid_rows = grid_latent.shape[1]
    nodes = mesh_latent.shape[1]
    edges = edge_source.shape[1]
    channels = grid_latent.shape[2]
    grid = grid_latent[0]
    cot = cotangent[0]
    live = (jnp.arange(edges, dtype=jnp.int32) < edge_count[0, 0]).astype(F32)[:, None]
    source_local = edge_source[0] - band * grid_rows
    dest_local = edge_dest[0] - (band - 1) * nodes

    width = w_qkv.shape[2]
    w_rows = jnp.concatenate([w_qkv.transpose(0, 2, 1).reshape(3 * width, channels), w_o], axis=0)
    w_mine = lax.all_gather(column_half(w_rows, core), MP, axis=0, tiled=True)
    cot_beside = lax.ppermute(cot, "mp_0", [(0, 1), (1, 0)])

    projected = dot(grid, w_in, NN)
    attr_columns = edge_attr[0].T
    attr_terms = sum(
        attr_columns[:, a : a + 1] * w_attr[a : a + 1] for a in range(w_attr.shape[0])
    )
    preact = projected[source_local] + attr_terms
    hidden = (jax.nn.silu(preact) * live).astype(BF)
    message = dot(hidden, w_out, NN).astype(BF)
    dest_table = (dest_local[:, None] == jnp.arange(3 * nodes, dtype=jnp.int32)[None, :]).astype(BF)
    partial_rows = dot(dest_table, message, TN)
    from_below = shifted(partial_rows[2 * nodes :].astype(BF), MP, 1)
    from_above = shifted(partial_rows[:nodes].astype(BF), MP, -1)
    node = (
        mesh_latent[0].astype(F32)
        + partial_rows[nodes : 2 * nodes]
        + from_below.astype(F32)
        + from_above.astype(F32)
    )
    inv = lax.rsqrt(jnp.mean(node * node, axis=-1, keepdims=True) + EPS)
    normed = (node * inv).astype(BF)

    normed_beside = lax.ppermute(normed, "mp_0", [(0, 1), (1, 0)])
    w_mine = after(w_mine, normed_beside)
    w_other = swapped(w_mine)
    both = jnp.concatenate([normed, cot], axis=0)
    heads = dot(column_half(both, core), w_mine, NT) + dot(column_half(both, 1 - core), w_other, NT)
    column = lax.broadcasted_iota(jnp.int32, (nodes, heads.shape[1]), 1)
    of_output = column % (4 * width) >= 3 * width
    heads = jnp.where(of_output, heads[nodes:], heads[:nodes]).astype(BF)
    heads = heads.reshape(nodes, bands, 4 * width).transpose(1, 0, 2)
    heads = lax.all_to_all(heads, MP, 0, 0, tiled=True).reshape(bands * nodes, 4 * width)

    wide = jnp.concatenate([normed, cot], axis=1)
    beside = jnp.concatenate([normed_beside, cot_beside], axis=1)
    wide = after(jnp.concatenate([wide, beside], axis=0), w_mine)
    wide = lax.all_gather(wide, "mp_1", axis=0, tiled=True)

    result, pieces = attend(heads, lax.axis_index("mp_0"), nodes)

    pieces = lax.all_to_all(pieces, MP, 0, 0, tiled=True)
    pieces = pieces.reshape(bands * 3 * width, nodes)

    def only_qkv(rows):
        rows = rows.reshape(bands, 4 * width, -1)[:, : 3 * width]
        return rows.reshape(bands * 3 * width, -1)

    dx = both_halves(
        dot(pieces, only_qkv(w_mine), TN), dot(pieces, only_qkv(w_other), TN), core
    )

    dnode = (
        cot.astype(F32)
        + inv * dx
        - node * inv * inv * inv * jnp.mean(dx * node, axis=-1, keepdims=True)
    )
    d_mesh = dnode.astype(BF)
    low = shifted(d_mesh, MP, 1)
    high = shifted(d_mesh, MP, -1)
    beside_all = jnp.concatenate([low, d_mesh, high], axis=0)
    dmessage = (beside_all[dest_local].astype(F32) * live).astype(BF)
    dw_out = dot(hidden, dmessage, TN).astype(BF)
    dhidden = dot(dmessage, w_out, NT)
    sigma = jax.nn.sigmoid(preact)
    dpre = dhidden * sigma * (1.0 + preact * (1.0 - sigma)) * live
    dw_attr = jnp.dot(
        edge_attr[0], dpre, precision=lax.Precision.HIGHEST, preferred_element_type=F32
    )
    source_table = (
        source_local[:, None] == jnp.arange(grid_rows, dtype=jnp.int32)[None, :]
    ).astype(BF)
    dproj = dot(source_table, dpre.astype(BF), TN).astype(BF)
    dw_in = dot(grid, dproj, TN).astype(BF)
    d_grid = dot(dproj, w_in, NT).astype(BF)

    dw_heads = dot(wide, result, (((0,), (1,)), ((), ()))).astype(BF)
    of_output = lax.broadcasted_iota(jnp.int32, (channels, 4 * width), 1) >= 3 * width
    dw_heads = jnp.where(of_output, dw_heads[channels:], dw_heads[:channels])

    rows = channels // (2 * groups)
    folded = 4 * width * rows // channels
    dw_heads = dw_heads.reshape(groups, 2, rows // folded, folded, 4 * width)
    dw_heads = dw_heads.transpose(0, 1, 3, 2, 4).reshape(groups, 2, folded, channels)
    both = jnp.concatenate(
        [
            dw_in.reshape(groups, 2, rows, channels),
            dw_out.reshape(groups, 2, rows, channels),
            dw_heads,
        ],
        axis=2,
    )
    mine = lax.dynamic_index_in_dim(both, core, 1, keepdims=False)
    theirs = lax.dynamic_index_in_dim(both, 1 - core, 1, keepdims=False)
    pair = mine.astype(F32) + swapped(theirs).astype(F32)
    pair = pair.astype(BF)
    attr = dw_attr + swapped(dw_attr)
    attr_rows = attr.shape[0]
    attr_high = attr.astype(BF)
    attr_low = (attr - attr_high.astype(F32)).astype(BF)
    blank = jnp.zeros((16 - 2 * attr_rows, channels), BF)
    tail = jnp.concatenate([attr_high, attr_low, blank], axis=0)
    pair = jnp.concatenate([pair, jnp.broadcast_to(tail[None], (groups, 16, channels))], axis=1)
    pair = lax.all_to_all(pair, GROUP, 0, 0, tiled=True)
    summed = jnp.sum(pair.astype(F32), axis=0)
    sum_heads = summed[2 * rows : 2 * rows + folded]
    sum_heads = sum_heads.reshape(folded, rows // folded, 4 * width).transpose(1, 0, 2)
    sum_heads = sum_heads.reshape(rows, 4 * width)
    sum_qkv = jnp.stack([sum_heads[:, j * width : (j + 1) * width] for j in range(3)])
    sum_o = sum_heads[:, 3 * width :].T
    first = 2 * rows + folded
    attr = summed[first : first + attr_rows] + summed[first + attr_rows : first + 2 * attr_rows]
    cols = channels // bands
    blocks = summed[: 2 * rows].astype(BF).reshape(2, rows, bands, cols)
    blocks = blocks.transpose(2, 1, 0, 3).reshape(bands, rows, 2 * cols)
    tail = attr.astype(BF).reshape(1, -1, 2 * cols)
    tail = jnp.broadcast_to(tail, (bands,) + tail.shape[1:])
    blocks = jnp.concatenate([blocks, tail], axis=1)
    blocks = lax.all_to_all(blocks, MP, 0, 0, tiled=True)
    summed = jnp.sum(blocks.astype(F32), axis=0)
    sum_in = summed[:rows, :cols]
    sum_out = summed[:rows, cols:]
    sum_attr = summed[rows:].reshape(attr.shape)
    return (d_grid[None], d_mesh[None], sum_attr, sum_in, sum_out, sum_qkv, sum_o)


def solution(mesh):
    finer = Mesh(mesh.devices.reshape(2, 4, 2, 2, 8), ("dp_0", "dp_1", "dp_2", "mp_0", "mp_1"))
    in_specs = (
        P(DP, MP, None),
        P(DP, MP, None),
        P(DP, MP),
        P(DP, MP),
        P(DP, MP),
        P(DP, None, MP),
        P(),
        P(),
        P(),
        P(None, None, MP),
        P(MP, None),
        P(DP, MP, None),
    )
    out_specs = (
        P(DP, MP, None),
        P(DP, MP, None),
        P(),
        P(DP, MP),
        P(DP, MP),
        P(None, DP, MP),
        P(MP, DP),
    )
    return jax.shard_map(
        shards, mesh=finer, in_specs=in_specs, out_specs=out_specs, check_vma=False
    )
```
